32 devices in a mesh: row: 4 (over x, core), col: 8 (over z, y).
Axes of the slice: x: 2, y: 2, z: 4, core: 2. Of those that a mesh axis runs over, the one named last changes fastest.
Arguments:
- tiles: bfloat16 [4, 8, 128, 128, 128], P('row', 'col')
- tile_row: int32 [4, 8, 128], P('row', 'col'), may hold values from 0 to 15, as said below
- tile_col: int32 [4, 8, 128], P('row', 'col'), may hold values from 0 to 15
- tile_count: int32 [4, 8], P('row', 'col'), may hold values from 1 to 128, as said below
- sinogram: float32 [4, 2048, 128], P('row', 'col')
Outputs:
- volume: float32 [8, 2048, 128], P('col', 'row')
- residual: float32 [4, 2048, 128], P('row', 'col')
The draws below stay inside these ranges and needn't reach their ends.
Inputs may be any that keep to these rules, and one draw needn't show every extreme that they name: Within one block the pairs (tile_row, tile_col) of all 128 slots are distinct. Slots 0 to tile_count - 1 of a block are live, the rest are ignored; some block has all 128 slots live in every draw.
All inputs are finite; a program needn't handle non-finite values.
Results may differ from the reference program's by a relative error of at most 0.015.
Values may be sent and summed in bfloat16 or wider, within the bound.
A program may use at most 64 MiB of HBM per device.

```python
import jax
import jax.numpy as jnp
from jax import lax

TILE = 128
RT = 16
VT = 16
TMAX = 128
FRAMES = 128
ITERS = 4
RAYS = 2048
VOX = 2048
N_ROW = 4
N_COL = 8


def tile_pairs(key):
    keys = jax.random.split(jax.random.fold_in(key, 7), N_ROW * N_COL)

    def shuffled(single):
        return jax.random.permutation(single, jnp.arange(RT * VT, dtype=jnp.int32))
    order = jax.vmap(shuffled)(keys)[:, :TMAX]
    rows = (order // VT).reshape(N_ROW, N_COL, TMAX).astype(jnp.int32)
    cols = (order % VT).reshape(N_ROW, N_COL, TMAX).astype(jnp.int32)
    return (rows, cols)


def draw_tile_row(key, part):
    return tile_pairs(key)[0]


def draw_tile_col(key, part):
    return tile_pairs(key)[1]


def draw_tile_count(key, part):
    base = TMAX // 8 + jax.random.randint(jax.random.fold_in(key, 3), (N_ROW * N_COL,), 0, TMAX // 2 + 1)
    base = jnp.maximum(base, 1)
    fullest = jax.random.randint(jax.random.fold_in(key, 5), (), 0, N_ROW * N_COL)
    base = jnp.where(jnp.arange(N_ROW * N_COL, dtype=jnp.int32) == fullest, TMAX, base)
    return base.reshape(N_ROW, N_COL).astype(jnp.int32)


def draw_tiles(key, part):
    shape = (N_ROW, N_COL, TMAX, TILE, TILE)
    place = lax_index(shape)
    rising = 3.0 ** (place / max(N_ROW * N_COL - 1, 1))
    fan = (TILE * N_COL * TMAX // (2 * RT)) ** (-0.5)
    values = jax.random.normal(jax.random.fold_in(key, 11), shape, jnp.float32)
    return (values * rising * fan).astype(jnp.bfloat16)


def lax_index(shape):
    first = jax.lax.broadcasted_iota(jnp.float32, shape, 0)
    second = jax.lax.broadcasted_iota(jnp.float32, shape, 1)
    return first * N_COL + second


def draw_sinogram(key, part):
    shape = (N_ROW, RAYS, FRAMES)
    ray = jax.lax.broadcasted_iota(jnp.float32, shape, 0) * RAYS + jax.lax.broadcasted_iota(jnp.float32, shape, 1)
    rising = 3.0 ** (ray / (N_ROW * RAYS - 1))
    values = jnp.clip(jax.random.normal(jax.random.fold_in(key, 17), shape, jnp.float32), -6.0, 6.0)
    return values * rising * 0.25


def setup_inputs(seed: int = 0) -> dict:
    key_of = jax.random.split(jax.random.key(seed), 6)
    return {
        "tiles": draw_tiles(jax.random.fold_in(key_of[5], 71), 0),
        "tile_row": draw_tile_row(jax.random.fold_in(key_of[5], 71), 0),
        "tile_col": draw_tile_col(jax.random.fold_in(key_of[5], 71), 0),
        "tile_count": draw_tile_count(jax.random.fold_in(key_of[5], 71), 0),
        "sinogram": draw_sinogram(jax.random.fold_in(key_of[5], 71), 0),
    }


def tile_pick(table, index):
    return lax.optimization_barrier(jnp.take(table, index, axis=0))


def forward_block(blocks, rows_index, cols_index, count, voxel_tiles):
    picked = tile_pick(voxel_tiles, cols_index)
    products = jnp.einsum("tij,tjk->tik", blocks.astype(jnp.float32), picked.astype(jnp.float32))
    live = jnp.arange(TMAX, dtype=jnp.int32) < count
    select = ((rows_index[None, :] == jnp.arange(RT, dtype=jnp.int32)[:, None]) & live[None, :]).astype(jnp.float32)
    return jnp.einsum("ut,tik->uik", select, products, precision=lax.Precision.HIGHEST)


def backward_block(blocks, rows_index, cols_index, count, ray_tiles):
    picked = tile_pick(ray_tiles, rows_index)
    products = jnp.einsum("tji,tjk->tik", blocks.astype(jnp.float32), picked.astype(jnp.float32))
    live = jnp.arange(TMAX, dtype=jnp.int32) < count
    select = ((cols_index[None, :] == jnp.arange(VT, dtype=jnp.int32)[:, None]) & live[None, :]).astype(jnp.float32)
    return jnp.einsum("ut,tik->uik", select, products, precision=lax.Precision.HIGHEST)


def reference(tiles, tile_row, tile_col, tile_count, sinogram):
    blocks_all = tiles.reshape(N_ROW * N_COL, TMAX, TILE, TILE)
    rows_all = tile_row.reshape(N_ROW * N_COL, TMAX)
    cols_all = tile_col.reshape(N_ROW * N_COL, TMAX)
    counts_all = tile_count.reshape(N_ROW * N_COL)
    devices = jnp.arange(N_ROW * N_COL, dtype=jnp.int32)

    def apply_forward(direction):
        voxel_tiles = direction.astype(jnp.bfloat16).reshape(N_COL, VT, TILE, FRAMES)

        def single(device):
            return forward_block(blocks_all[device], rows_all[device], cols_all[device],
                                 counts_all[device], voxel_tiles[device % N_COL])

        parts = lax.map(single, devices)
        return parts.reshape(N_ROW, N_COL, RAYS, FRAMES).sum(axis=1)

    def apply_backward(field):
        ray_tiles = field.astype(jnp.bfloat16).reshape(N_ROW, RT, TILE, FRAMES)

        def single(device):
            return backward_block(blocks_all[device], rows_all[device], cols_all[device],
                                  counts_all[device], ray_tiles[device // N_COL])

        parts = lax.map(single, devices)
        return parts.reshape(N_ROW, N_COL, VOX, FRAMES).sum(axis=0)

    volume = jnp.zeros((N_COL, VOX, FRAMES), jnp.float32)
    residual = sinogram
    search = apply_backward(residual)
    gamma = jnp.sum(search * search, axis=(0, 1))
    direction = search
    for step in range(ITERS):
        image = apply_forward(direction)
        alpha = gamma / jnp.sum(image * image, axis=(0, 1))
        volume = volume + alpha * direction
        residual = residual - alpha * image
        if step + 1 < ITERS:
            search = apply_backward(residual)
            fresh = jnp.sum(search * search, axis=(0, 1))
            direction = search + (fresh / gamma) * direction
            gamma = fresh
    return volume, residual
```

```python
import functools

import jax
import jax.numpy as jnp
from jax import lax
from jax.experimental import pallas as pl
from jax.experimental.pallas import tpu as pltpu
from jax.sharding import PartitionSpec as P

RT = 16
VT = 16
ITERS = 4
CORES = 2
PIECE = 256
AXIS_REFS = 15
MESH = pl.DeviceIdType.MESH
F32 = jnp.float32
BF16 = jnp.bfloat16


def inner_size(n):
    size = 1
    while size * 2 * size * 2 <= n and n % (size * 2) == 0:
        size *= 2
    return size


def build(slot_ref, tiles, dense, flipped, start, stop):
    tile = tiles.shape[1]
    group = 4

    def place(step, carry):
        for j in range(group):
            at = step * group + j
            r = pl.multiple_of(at // VT * tile, tile)
            c = pl.multiple_of(lax.rem(at, VT) * tile, tile)
            block = tiles[slot_ref[at]]
            dense[pl.ds(r, tile), pl.ds(c, tile)] = block
            flipped[pl.ds(c, tile), pl.ds(r, tile)] = block.T
        return carry

    lax.fori_loop(start // group, stop // group, place, 0)


class Axis:
    def __init__(self, name, n, n_in, chunk, refs):
        self.name, self.n, self.n_in, self.n_out, self.chunk = name, n, n_in, n // n_in, chunk
        self.near_out, self.near_in, self.far_out, self.far_in, self.norm_in = refs[:5]
        (self.near_ss, self.near_rs, self.far_ss, self.far_rs, self.out_ss, self.out_rs,
         self.in_ss, self.in_rs, self.norm_ss, self.norm_rs) = refs[5:]
        self.me = lax.axis_index(name)
        self.o, self.i = self.me // n_in, lax.rem(self.me, n_in)

    def index(self, e, d):
        return lax.rem(self.o + e + self.n_out, self.n_out) * self.n_in + lax.rem(self.i + d + self.n_in, self.n_in)

    def rows(self, index):
        return pl.ds(pl.multiple_of(index * self.chunk, self.chunk), self.chunk)

    def send(self, src, dst, ss, rs, index):
        copy = pltpu.make_async_remote_copy(
            src_ref=src, dst_ref=dst, send_sem=ss, recv_sem=rs,
            device_id={self.name: index}, device_id_type=MESH,
        )
        copy.start()
        return copy

    def outer_order(self):
        return sorted(range(1, self.n_out), key=lambda e: -min(e, self.n_out - e)) + [0]

    def reduce_scatter(self, matrix, full, queued=lambda: None):
        def piece(index):
            return jnp.dot(matrix[self.rows(index), :], full[...], preferred_element_type=F32)

        copies = []
        near = {}
        for e in self.outer_order():
            for d in range(1, self.n_in):
                self.near_out[d - 1, e] = piece(self.index(e, d)).astype(BF16)
                near[e, d] = self.send(
                    self.near_out.at[d - 1, e], self.near_in.at[d - 1, e],
                    self.near_ss.at[d - 1, e], self.near_rs.at[d - 1, e], self.index(0, d))
        queued()
        far = {}
        total = None
        for e in self.outer_order():
            total = piece(self.index(e, 0))
            for d in range(1, self.n_in):
                near[e, d].wait_recv()
                total += self.near_in[d - 1, e].astype(F32)
            if e:
                self.far_out[e - 1] = total.astype(BF16)
                far[e] = self.send(
                    self.far_out.at[e - 1], self.far_in.at[e - 1],
                    self.far_ss.at[e - 1], self.far_rs.at[e - 1], self.index(e, 0))
        for e in far:
            far[e].wait_recv()
            total += self.far_in[e - 1].astype(F32)
        for copy in list(near.values()) + list(far.values()):
            copy.wait_send()
        return total

    def all_gather(self, value, full, between=lambda step: None):
        full[self.rows(self.me), :] = value.astype(BF16)
        mine = full.at[self.rows(self.me), :]
        far, near = {}, {}
        for e in reversed(self.outer_order()[:-1]):
            far[e] = self.send(mine, mine, self.out_ss.at[e - 1], self.out_rs.at[e - 1], self.index(e, 0))
        for d in range(1, self.n_in):
            near[0, d] = self.send(mine, mine, self.in_ss.at[d - 1, 0], self.in_rs.at[d - 1, 0], self.index(0, d))
        between(0)
        for step, e in enumerate(reversed(self.outer_order()[:-1])):
            far[e].wait_recv()
            theirs = full.at[self.rows(self.index(-e, 0)), :]
            for d in range(1, self.n_in):
                near[e, d] = self.send(
                    theirs, theirs, self.in_ss.at[d - 1, e], self.in_rs.at[d - 1, e], self.index(0, d))
            between(step + 1)
        for copy in near.values():
            copy.wait_recv()
        for copy in list(near.values()) + list(far.values()):
            copy.wait_send()

    def peer(self, d):
        return lax.rem(self.me + d, self.n)

    def norm_send(self, value, which):
        self.norm_in[which, 0] = jnp.broadcast_to(value, self.norm_in.shape[2:])
        return [
            self.send(self.norm_in.at[which, 0], self.norm_in.at[which, d],
                      self.norm_ss.at[which, d - 1], self.norm_rs.at[which, d - 1], self.peer(d))
            for d in range(1, self.n)
        ]

    def norm_wait(self, which):
        for d in range(1, self.n):
            pltpu.make_async_remote_copy(
                src_ref=self.norm_in.at[which, 0], dst_ref=self.norm_in.at[which, d],
                send_sem=self.norm_ss.at[which, d - 1], recv_sem=self.norm_rs.at[which, d - 1],
                device_id={self.name: self.peer(d)}, device_id_type=MESH,
            ).wait()
        total = self.norm_in[which, 0]
        for d in range(1, self.n):
            total += self.norm_in[which, d]
        return total[0:1, :]


class Exchange:
    def __init__(self, axis, pieces, refs):
        self.axis, self.pieces = axis, pieces
        self.near_out, self.near_in, self.far_out, self.far_in = refs[:4]
        self.near_ss, self.near_rs, self.far_ss, self.far_rs, self.back_ss, self.back_rs = refs[4:]

    def rows(self, core, at, size):
        chunk = self.axis.chunk
        start = (at // chunk * self.axis.n_in + core) * chunk + at % chunk
        return pl.ds(pl.multiple_of(start, size), size)

    def run(self, matrix, full, total, own):
        axis = self.axis
        mine, other = axis.i, 1 - axis.i
        near_peer, far_peer = axis.index(0, 1), axis.index(1, 0)

        def piece(core, at, size):
            return jnp.dot(matrix[self.rows(core, at, size), :], full[...], preferred_element_type=F32)

        def give(p):
            at, size = self.pieces[p]
            self.near_out[pl.ds(at, size)] = piece(other, at, size).astype(BF16)
            return axis.send(self.near_out.at[pl.ds(at, size)], self.near_in.at[pl.ds(at, size)],
                             self.near_ss.at[p], self.near_rs.at[p], near_peer)

        count = len(self.pieces)
        near, far, back = [give(0)], [], []
        for p, (at, size) in enumerate(self.pieces):
            if p + 1 < count:
                near.append(give(p + 1))
            part = piece(mine, at, size)
            near[p].wait_recv()
            here = pl.ds(at, size)
            self.far_out[here] = (part + self.near_in[here].astype(F32)).astype(BF16)
            far.append(axis.send(self.far_out.at[here], self.far_in.at[here],
                                 self.far_ss.at[p], self.far_rs.at[p], far_peer))
        for p, (at, size) in enumerate(self.pieces):
            far[p].wait_recv()
            here = pl.ds(at, size)
            rows = self.rows(mine, at, size)
            value = self.far_out[here].astype(F32) + self.far_in[here].astype(F32)
            total[rows] = value.astype(BF16)
            back.append(axis.send(total.at[rows], total.at[rows], self.back_ss.at[p], self.back_rs.at[p], near_peer))
        start = pl.multiple_of(axis.o * axis.chunk, axis.chunk)
        here = pl.ds(start, axis.chunk)
        own[...] = self.far_out[here].astype(F32) + self.far_in[here].astype(F32)
        for copy in back:
            copy.wait_recv()
        for copy in near + far + back:
            copy.wait_send()


def squares(ref, step):
    total = None
    for at in range(0, ref.shape[0], step):
        part = ref[at:at + step, :].astype(F32)
        part = jnp.sum(part * part, axis=0, keepdims=True)
        total = part if total is None else total + part
    return total


def cgls_kernel(sizes, slot_ref, tiles_hbm, sino_ref, volume_ref, residual_ref, tiles, dense, flipped, rays, voxels,
                images, held, search, direction, image, gamma, guess, load_sem, *refs):
    n_row, n_col, col_in, pieces = sizes
    row = Axis("row", n_row, CORES, search.shape[0], refs[:AXIS_REFS])
    col = Axis("col", n_col, col_in, image.shape[0], refs[AXIS_REFS:2 * AXIS_REFS])
    exchange = Exchange(row, pieces, refs[2 * AXIS_REFS:]) if pieces else None

    slots = tiles_hbm.shape[0]
    load = pltpu.make_async_copy(tiles_hbm, tiles.at[pl.ds(0, slots)], load_sem)
    load.start()
    tiles[slots] = jnp.zeros(tiles.shape[1:], tiles.dtype)

    barrier = pltpu.get_barrier_semaphore()
    for axis in (row, col):
        for d in range(1, axis.n):
            pl.semaphore_signal(barrier, inc=1, device_id={axis.name: axis.peer(d)}, device_id_type=MESH)
    pl.semaphore_wait(barrier, n_row + n_col - 2)

    share = RT * VT // col.n_out

    def build_share(step):
        if step == 0:
            load.wait()
        build(slot_ref, tiles, dense, flipped, step * share, (step + 1) * share)

    col.all_gather(sino_ref[...], rays, build_share)
    held[...] = rays[...].astype(F32)
    residual_ref[...] = sino_ref[...]
    volume_ref[...] = jnp.zeros_like(volume_ref)
    direction[...] = jnp.zeros_like(direction)
    image[...] = jnp.zeros_like(image)
    gamma[...] = jnp.ones_like(gamma)
    row.norm_send(squares(rays, 256), 1)

    def iteration(k, carry):
        if exchange:
            exchange.run(flipped, rays, voxels, search)
        else:
            search[...] = row.reduce_scatter(flipped, rays)
            row.all_gather(search[...], voxels)

        @pl.when(k == 0)
        def _():
            guess[...] = row.norm_wait(1)

        forth = col.reduce_scatter(dense, voxels, lambda: col.norm_send(squares(voxels, 256), 0))
        fresh = col.norm_wait(0)
        beta = jnp.where(k > 0, fresh / gamma[...], jnp.zeros_like(fresh))
        gamma[...] = fresh
        image[...] = forth + beta * image[...]
        col.norm_send(squares(image, image.shape[0]), 1)
        likely = jnp.where(k > 0, guess[...], guess[...] / fresh)

        @pl.when(k + 1 < ITERS)
        def _():
            def norm_on(step):
                if step == col.n_out - 1:
                    row.norm_send(col.norm_wait(1), 0)

            col.all_gather(residual_ref[...] - likely * image[...], images, norm_on)

        @pl.when(k + 1 == ITERS)
        def _():
            row.norm_send(col.norm_wait(1), 0)

        direction[...] = search[...] + beta * direction[...]
        alpha = fresh / row.norm_wait(0)
        guess[...] = 1.25 * alpha

        @pl.when(k + 1 < ITERS)
        def _():
            held[...] += alpha / likely * (images[...].astype(F32) - held[...])
            rays[...] = held[...].astype(BF16)

        residual_ref[...] -= alpha * image[...]
        volume_ref[...] += alpha * direction[...]
        return carry

    lax.fori_loop(0, ITERS, iteration, 0)


def axis_scratch(n, n_in, chunk, frames):
    n_out = n // n_in
    dma = pltpu.SemaphoreType.DMA
    near, far = (max(n_in - 1, 1), n_out), (max(n_out - 1, 1),)
    return [
        pltpu.VMEM(near + (chunk, frames), BF16),
        pltpu.VMEM(near + (chunk, frames), BF16),
        pltpu.VMEM(far + (chunk, frames), BF16),
        pltpu.VMEM(far + (chunk, frames), BF16),
        pltpu.VMEM((2, n, 8, frames), F32),
        dma(near), dma(near), dma(far), dma(far), dma(far), dma(far), dma(near), dma(near),
        dma((2, n - 1)), dma((2, n - 1)),
    ]


def exchange_scratch(count, rows, frames):
    buffer = pltpu.VMEM((rows, frames), BF16)
    return [buffer] * 4 + [pltpu.SemaphoreType.DMA((count,))] * 6


def local(n_row, n_col, tiles, tile_row, tile_col, tile_count, sinogram):
    tile, frames = tiles.shape[3], sinogram.shape[2]
    n_rays, n_vox = RT * tile, VT * tile
    vmem = pl.BlockSpec(memory_space=pltpu.VMEM)
    smem = pl.BlockSpec(memory_space=pltpu.SMEM)
    slots = tiles.shape[2]
    slot = jnp.arange(slots, dtype=jnp.int32)
    place = tile_row[0, 0] * VT + tile_col[0, 0]
    match = (place[None, :] == jnp.arange(RT * VT, dtype=jnp.int32)[:, None]) & (slot[None, :] < tile_count[0, 0])
    slot_of = jnp.min(jnp.where(match, slot[None, :], slots), axis=1)

    col_in = inner_size(n_col)
    vox_piece, ray_piece = n_vox // n_row, n_rays // n_col
    pieces = []
    if n_row == 2 * CORES:
        step = min(PIECE, vox_piece)
        pieces = [(at, step) for at in range(0, 2 * vox_piece, step)]
    hbm = pl.BlockSpec(memory_space=pl.ANY)
    volume, residual = pl.pallas_call(
        functools.partial(cgls_kernel, (n_row, n_col, col_in, pieces)),
        out_shape=(
            jax.ShapeDtypeStruct((vox_piece, frames), F32),
            jax.ShapeDtypeStruct((ray_piece, frames), F32),
        ),
        in_specs=[smem, hbm, vmem],
        out_specs=(vmem, vmem),
        scratch_shapes=[
            pltpu.VMEM((slots + 1, tile, tile), BF16),
            pltpu.VMEM((n_rays, n_vox), BF16),
            pltpu.VMEM((n_vox, n_rays), BF16),
            pltpu.VMEM((n_rays, frames), BF16),
            pltpu.VMEM((n_vox, frames), BF16),
            pltpu.VMEM((n_rays, frames), BF16),
            pltpu.VMEM((n_rays, frames), F32),
            pltpu.VMEM((vox_piece, frames), F32),
            pltpu.VMEM((vox_piece, frames), F32),
            pltpu.VMEM((ray_piece, frames), F32),
            pltpu.VMEM((1, frames), F32),
            pltpu.VMEM((1, frames), F32),
            pltpu.SemaphoreType.DMA,
        ]
        + axis_scratch(n_row, CORES, vox_piece, frames)
        + axis_scratch(n_col, col_in, ray_piece, frames)
        + (exchange_scratch(len(pieces), 2 * vox_piece, frames) if pieces else []),
        compiler_params=pltpu.CompilerParams(
            collective_id=0, has_side_effects=True, vmem_limit_bytes=62 * 1024 * 1024
        ),
        name="cgls",
    )(slot_of, tiles[0, 0], sinogram[0])
    return volume[None], residual[None]


def solution(mesh):
    return jax.shard_map(
        functools.partial(local, mesh.shape["row"], mesh.shape["col"]),
        mesh=mesh,
        in_specs=(
            P("row", "col", None, None, None),
            P("row", "col", None),
            P("row", "col", None),
            P("row", "col"),
            P("row", "col", None),
        ),
        out_specs=(P("col", "row", None), P("row", "col", None)),
        check_vma=False,
    )
```

```python
import functools

import jax
import jax.numpy as jnp
from jax import lax
from jax.experimental import pallas as pl
from jax.experimental.pallas import tpu as pltpu
from jax.sharding import PartitionSpec as P

RT = 16
VT = 16
ITERS = 4
CORES = 2
PIECE = 256
PARTS = 2
AXIS_REFS = 15
LINE_REFS = 17
MESH = pl.DeviceIdType.MESH
F32 = jnp.float32
BF16 = jnp.bfloat16


def inner_size(n):
    size = 1
    while size * 2 * size * 2 <= n and n % (size * 2) == 0:
        size *= 2
    return size


def build(slot_ref, tiles, dense, flipped, start, stop):
    tile = tiles.shape[1]
    group = 4

    def place(step, carry):
        for j in range(group):
            at = step * group + j
            r = pl.multiple_of(at // VT * tile, tile)
            c = pl.multiple_of(lax.rem(at, VT) * tile, tile)
            block = tiles[slot_ref[at // slot_ref.shape[2], 0, lax.rem(at, slot_ref.shape[2])]]
            dense[pl.ds(r, tile), pl.ds(c, tile)] = block
            flipped[pl.ds(c, tile), pl.ds(r, tile)] = block.T
        return carry

    lax.fori_loop(start // group, stop // group, place, 0)


class Axis:
    def __init__(self, name, n, n_in, chunk, refs):
        self.name, self.n, self.n_in, self.n_out, self.chunk = name, n, n_in, n // n_in, chunk
        self.near_out, self.near_in, self.far_out, self.far_in, self.norm_in = refs[:5]
        (self.near_ss, self.near_rs, self.far_ss, self.far_rs, self.out_ss, self.out_rs,
         self.in_ss, self.in_rs, self.norm_ss, self.norm_rs) = refs[5:]
        self.me = lax.axis_index(name)
        self.o, self.i = self.me // n_in, lax.rem(self.me, n_in)

    def index(self, e, d):
        return lax.rem(self.o + e + self.n_out, self.n_out) * self.n_in + lax.rem(self.i + d + self.n_in, self.n_in)

    def rows(self, index):
        return pl.ds(pl.multiple_of(index * self.chunk, self.chunk), self.chunk)

    def send(self, src, dst, ss, rs, index):
        copy = pltpu.make_async_remote_copy(
            src_ref=src, dst_ref=dst, send_sem=ss, recv_sem=rs,
            device_id={self.name: index}, device_id_type=MESH,
        )
        copy.start()
        return copy

    def outer_order(self):
        return sorted(range(1, self.n_out), key=lambda e: -min(e, self.n_out - e)) + [0]

    def reduce_scatter(self, matrix, full, queued=lambda: None):
        def piece(index):
            return jnp.dot(matrix[self.rows(index), :], full[...], preferred_element_type=F32)

        copies = []
        near = {}
        for e in self.outer_order():
            for d in range(1, self.n_in):
                self.near_out[d - 1, e] = piece(self.index(e, d)).astype(BF16)
                near[e, d] = self.send(
                    self.near_out.at[d - 1, e], self.near_in.at[d - 1, e],
                    self.near_ss.at[d - 1, e], self.near_rs.at[d - 1, e], self.index(0, d))
        queued()
        far = {}
        total = None
        for e in self.outer_order():
            total = piece(self.index(e, 0))
            for d in range(1, self.n_in):
                near[e, d].wait_recv()
                total += self.near_in[d - 1, e].astype(F32)
            if e:
                self.far_out[e - 1] = total.astype(BF16)
                far[e] = self.send(
                    self.far_out.at[e - 1], self.far_in.at[e - 1],
                    self.far_ss.at[e - 1], self.far_rs.at[e - 1], self.index(e, 0))
        for e in far:
            far[e].wait_recv()
            total += self.far_in[e - 1].astype(F32)
        for copy in list(near.values()) + list(far.values()):
            copy.wait_send()
        return total

    def all_gather(self, value, full, between=lambda step: None):
        full[self.rows(self.me), :] = value.astype(BF16)
        mine = full.at[self.rows(self.me), :]
        far, near = {}, {}
        for e in reversed(self.outer_order()[:-1]):
            far[e] = self.send(mine, mine, self.out_ss.at[e - 1], self.out_rs.at[e - 1], self.index(e, 0))
        for d in range(1, self.n_in):
            near[0, d] = self.send(mine, mine, self.in_ss.at[d - 1, 0], self.in_rs.at[d - 1, 0], self.index(0, d))
        between(0)
        for step, e in enumerate(reversed(self.outer_order()[:-1])):
            far[e].wait_recv()
            theirs = full.at[self.rows(self.index(-e, 0)), :]
            for d in range(1, self.n_in):
                near[e, d] = self.send(
                    theirs, theirs, self.in_ss.at[d - 1, e], self.in_rs.at[d - 1, e], self.index(0, d))
            between(step + 1)
        for copy in near.values():
            copy.wait_recv()
        for copy in list(near.values()) + list(far.values()):
            copy.wait_send()

    def peer(self, d):
        return lax.rem(self.me + d, self.n)

    def norm_send(self, value, which):
        self.norm_in[which, 0] = value
        return [
            self.send(self.norm_in.at[which, 0], self.norm_in.at[which, d],
                      self.norm_ss.at[which, d - 1], self.norm_rs.at[which, d - 1], self.peer(d))
            for d in range(1, self.n)
        ]

    def norm_wait(self, which):
        for d in range(1, self.n):
            pltpu.make_async_remote_copy(
                src_ref=self.norm_in.at[which, 0], dst_ref=self.norm_in.at[which, d],
                send_sem=self.norm_ss.at[which, d - 1], recv_sem=self.norm_rs.at[which, d - 1],
                device_id={self.name: self.peer(d)}, device_id_type=MESH,
            ).wait()
        total = self.norm_in[which, 0]
        for d in range(1, self.n):
            total += self.norm_in[which, d]
        return total


class Line(Axis):
    def __init__(self, name, n, n_in, chunk, refs):
        self.near_out, self.near_in, self.far_out, self.far_in, self.norm_in, self.hold, self.total = refs[:7]
        (self.near_ss, self.near_rs, self.far_ss, self.far_rs, self.out_ss, self.out_rs,
         self.in_ss, self.in_rs, self.norm_ss, self.norm_rs) = refs[7:]
        self.name, self.n, self.n_in, self.n_out, self.chunk = name, n, n_in, n // n_in, chunk
        self.me = lax.axis_index(name)
        self.o, self.i = self.me // n_in, lax.rem(self.me, n_in)
        low = self.o < 2
        self.edge = (self.o == 0) | (self.o == 3)
        self.inner = jnp.logical_not(self.edge)
        self.outer = [self.o, jnp.where(low, 1 - self.o, 5 - self.o), jnp.where(low, 2, 1), jnp.where(low, 3, 0)]
        self.part = chunk // PARTS

    def at(self, place, d=0):
        return self.outer[place] * self.n_in + lax.rem(self.i + d, self.n_in)

    def span(self, h):
        return pl.ds(h * self.part, self.part)

    def block(self, full, place, h):
        start = pl.multiple_of(self.at(place) * self.chunk + h * self.part, self.part)
        return full.at[pl.ds(start, self.part), :]

    def link(self, src, dst, ss, rs, index):
        return pltpu.make_async_remote_copy(
            src_ref=src, dst_ref=dst, send_sem=ss, recv_sem=rs,
            device_id={self.name: index}, device_id_type=MESH,
        )

    def reduce_scatter(self, matrix, full, queued=lambda: None):
        def piece(index):
            return jnp.dot(matrix[self.rows(index), :], full[...], preferred_element_type=F32)

        parts, others = range(PARTS), range(1, self.n_in)
        sent = []
        for place in (3, 2, 1, 0):
            for d in others:
                self.near_out[d - 1, place] = piece(self.at(place, d)).astype(BF16)
                for h in parts:
                    copy = self.link(self.near_out.at[d - 1, place, self.span(h)],
                                     self.near_in.at[d - 1, place, self.span(h)],
                                     self.near_ss.at[d - 1, place, h], self.near_rs.at[d - 1, place, h],
                                     self.at(0, d))
                    copy.start()
                    sent.append(copy)
        queued()

        def gathered(place, h):
            part = self.hold[self.span(h)]
            for d in others:
                self.link(self.near_out.at[d - 1, place, self.span(h)], self.near_in.at[d - 1, place, self.span(h)],
                          self.near_ss.at[d - 1, place, h], self.near_rs.at[d - 1, place, h],
                          self.at(0, d)).wait_recv()
                part += self.near_in[d - 1, place, self.span(h)].astype(F32)
            return part

        def far(which, slot, h, place):
            return self.link(self.far_out.at[which, self.span(h)], self.far_in.at[slot, self.span(h)],
                             self.far_ss.at[which, h], self.far_rs.at[slot, h], self.at(place))

        self.hold[...] = piece(self.at(3))
        for h in parts:
            self.hold[self.span(h)] = gathered(3, h)

            @pl.when(self.edge)
            def _():
                self.far_out[2, self.span(h)] = self.hold[self.span(h)].astype(BF16)
                far(2, 3, h, 1).start()

        self.total[...] = self.hold[...]
        self.hold[...] = piece(self.at(2))
        for h in parts:
            self.far_out[1, self.span(h)] = gathered(2, h).astype(BF16)
            far(1, jnp.where(self.edge, 2, 1), h, 2).start()
        self.hold[...] = piece(self.at(1))

        @pl.when(self.inner)
        def _():
            for h in parts:
                far(2, 3, h, 1).wait_recv()
                value = self.total[self.span(h)] + self.far_in[3, self.span(h)].astype(F32)
                self.far_out[2, self.span(h)] = value.astype(BF16)
                far(2, 1, h, 3).start()

        for h in parts:
            self.far_out[0, self.span(h)] = gathered(1, h).astype(BF16)
            far(0, 0, h, 1).start()
        self.hold[...] = piece(self.at(0))
        for h in parts:
            self.hold[self.span(h)] = gathered(0, h)
        for h in parts:
            far(0, 0, h, 1).wait_recv()
            self.hold[self.span(h)] += self.far_in[0, self.span(h)].astype(F32)

        @pl.when(self.inner)
        def _():
            for h in parts:
                far(1, 2, h, 2).wait_recv()
                self.hold[self.span(h)] += self.far_in[2, self.span(h)].astype(F32)

        for h in parts:
            far(1, 1, h, 2).wait_recv()
            self.hold[self.span(h)] += self.far_in[1, self.span(h)].astype(F32)
        for copy in sent:
            copy.wait_send()
        for which in range(3):
            for h in parts:
                far(which, 0, h, 1).wait_send()
        return self.hold[...]

    def all_gather(self, value, full, between=lambda step: None):
        parts, others = range(PARTS), range(1, self.n_in)
        full[self.rows(self.me), :] = value.astype(BF16)

        def pass_on(place, slot, to, sem, h):
            block = self.block(full, place, h)
            return self.link(block, block, self.out_ss.at[sem, h], self.out_rs.at[slot - 1, h], self.at(to))

        def arrived(place, h):
            block = self.block(full, place, h)
            self.link(block, block, self.out_ss.at[0, h], self.out_rs.at[place - 1, h], self.at(1)).wait_recv()

        def share(place, h):
            block = self.block(full, place, h)
            return [self.link(block, block, self.in_ss.at[d - 1, place, h], self.in_rs.at[d - 1, place, h],
                              self.at(0, d)) for d in others]

        def spread(place, h):
            for copy in share(place, h):
                copy.start()

        @pl.when(self.edge)
        def _():
            for h in parts:
                pass_on(0, 3, 3, 0, h).start()
            for h in parts:
                pass_on(0, 1, 1, 2, h).start()
                pass_on(0, 3, 2, 1, h).start()

        @pl.when(self.inner)
        def _():
            for h in parts:
                pass_on(0, 2, 2, 0, h).start()
                pass_on(0, 1, 1, 1, h).start()

        for h in parts:
            spread(0, h)
        between(0)

        @pl.when(self.inner)
        def _():
            for h in parts:
                arrived(2, h)
                pass_on(2, 2, 1, 2, h).start()
                spread(2, h)

        for h in parts:
            arrived(1, h)
            spread(1, h)
        between(1)
        for h in parts:
            arrived(3, h)
            spread(3, h)
        between(2)

        @pl.when(self.edge)
        def _():
            for h in parts:
                arrived(2, h)
                spread(2, h)

        between(3)
        for place in range(4):
            for h in parts:
                for copy in share(place, h):
                    copy.wait()
        for sem in range(3):
            for h in parts:
                pass_on(0, 1, 1, sem, h).wait_send()


class World:
    def __init__(self, row, col, refs):
        self.row, self.col = row, col
        self.got, self.ss, self.rs = refs

    def peers(self):
        for at in range(1, self.row.n * self.col.n):
            a, b = at // self.col.n, at % self.col.n
            yield at, {self.row.name: self.row.peer(a), self.col.name: self.col.peer(b)}

    def copy(self, at, device):
        return pltpu.make_async_remote_copy(
            src_ref=self.got.at[0], dst_ref=self.got.at[at], send_sem=self.ss.at[at - 1],
            recv_sem=self.rs.at[at - 1], device_id=device, device_id_type=MESH)

    def send(self, value):
        self.got[0] = value
        for at, device in self.peers():
            self.copy(at, device).start()

    def wait(self):
        for at, device in self.peers():
            self.copy(at, device).wait()
        return jnp.sum(self.got[...], axis=0)


class Exchange:
    def __init__(self, axis, pieces, refs):
        self.axis, self.pieces = axis, pieces
        self.near_out, self.near_in, self.far_out, self.far_in = refs[:4]
        self.near_ss, self.near_rs, self.far_ss, self.far_rs, self.back_ss, self.back_rs = refs[4:]

    def rows(self, core, at, size):
        chunk = self.axis.chunk
        start = (at // chunk * self.axis.n_in + core) * chunk + at % chunk
        return pl.ds(pl.multiple_of(start, size), size)

    def run(self, matrix, full, total, own):
        axis = self.axis
        mine, other = axis.i, 1 - axis.i
        near_peer, far_peer = axis.index(0, 1), axis.index(1, 0)

        def piece(core, at, size):
            return jnp.dot(matrix[self.rows(core, at, size), :], full[...], preferred_element_type=F32)

        def give(p):
            at, size = self.pieces[p]
            self.near_out[pl.ds(at, size)] = piece(other, at, size).astype(BF16)
            return axis.send(self.near_out.at[pl.ds(at, size)], self.near_in.at[pl.ds(at, size)],
                             self.near_ss.at[p], self.near_rs.at[p], near_peer)

        count = len(self.pieces)
        near, far, back = [give(0)], [], []
        for p, (at, size) in enumerate(self.pieces):
            if p + 1 < count:
                near.append(give(p + 1))
            part = piece(mine, at, size)
            near[p].wait_recv()
            here = pl.ds(at, size)
            self.far_out[here] = (part + self.near_in[here].astype(F32)).astype(BF16)
            far.append(axis.send(self.far_out.at[here], self.far_in.at[here],
                                 self.far_ss.at[p], self.far_rs.at[p], far_peer))
        for p, (at, size) in enumerate(self.pieces):
            far[p].wait_recv()
            here = pl.ds(at, size)
            rows = self.rows(mine, at, size)
            value = self.far_out[here].astype(F32) + self.far_in[here].astype(F32)
            total[rows] = value.astype(BF16)
            back.append(axis.send(total.at[rows], total.at[rows], self.back_ss.at[p], self.back_rs.at[p], near_peer))
        start = pl.multiple_of(axis.o * axis.chunk, axis.chunk)
        here = pl.ds(start, axis.chunk)
        own[...] = self.far_out[here].astype(F32) + self.far_in[here].astype(F32)
        for copy in back:
            copy.wait_recv()
        for copy in near + far + back:
            copy.wait_send()


def squares(ref, step):
    total = None
    for at in range(0, ref.shape[0], step):
        part = ref[at:at + step, :].astype(F32)
        part = jnp.sum(part * part, axis=0, keepdims=True)
        total = part if total is None else total + part
    return total


def cgls_kernel(sizes, count_ref, row_ref, col_ref, tiles_hbm, sino_ref, volume_ref, residual_ref, tiles, dense, flipped, rays, voxels,
                images, held, search, direction, image, gamma, guess, ratio, load_sem, table, slot_ref, table_sem, *refs):
    n_row, n_col, col_in, pieces = sizes
    row = Axis("row", n_row, CORES, search.shape[0], refs[:AXIS_REFS])
    kind, count = (Line, LINE_REFS) if n_col == 4 * col_in else (Axis, AXIS_REFS)
    col = kind("col", n_col, col_in, image.shape[0], refs[AXIS_REFS:AXIS_REFS + count])
    refs = refs[AXIS_REFS + count:]
    world = World(row, col, refs[:3])
    exchange = Exchange(row, pieces, refs[3:]) if pieces else None

    slots = tiles_hbm.shape[0]
    load = pltpu.make_async_copy(tiles_hbm, tiles.at[pl.ds(0, slots)], load_sem)
    load.start()
    tiles[slots] = jnp.zeros(tiles.shape[1:], tiles.dtype)

    place = (row_ref[...] * VT + col_ref[...]).astype(F32)
    place = jnp.broadcast_to(place, (slots, slots)).T
    slot = lax.broadcasted_iota(jnp.int32, (slots, slots), 0)
    lane = lax.broadcasted_iota(jnp.int32, (slots, slots), 1).astype(F32)
    for at in range(0, RT * VT, slots):
        live = (place == lane + at) & (slot < count_ref[...])
        table[at // slots] = jnp.min(jnp.where(live, slot, slots), axis=0, keepdims=True)
    fill = pltpu.make_async_copy(table, slot_ref, table_sem)
    fill.start()

    barrier = pltpu.get_barrier_semaphore()
    for axis in (row, col):
        for d in range(1, axis.n):
            pl.semaphore_signal(barrier, inc=1, device_id={axis.name: axis.peer(d)}, device_id_type=MESH)
    pl.semaphore_wait(barrier, n_row + n_col - 2)

    share = RT * VT // col.n_out

    def build_share(step):
        if step == 0:
            load.wait()
            fill.wait()
        build(slot_ref, tiles, dense, flipped, step * share, (step + 1) * share)

    col.all_gather(sino_ref[...], rays, build_share)
    held[...] = rays[...].astype(F32)
    residual_ref[...] = sino_ref[...]
    volume_ref[...] = jnp.zeros_like(volume_ref)
    direction[...] = jnp.zeros_like(direction)
    image[...] = jnp.zeros_like(image)
    gamma[...] = jnp.ones_like(gamma)
    row.norm_send(squares(rays, 256), 1)

    def iteration(k, carry):
        if exchange:
            exchange.run(flipped, rays, voxels, search)
        else:
            search[...] = row.reduce_scatter(flipped, rays)
            row.all_gather(search[...], voxels)

        @pl.when(k == 0)
        def _():
            guess[...] = row.norm_wait(1)

        forth = col.reduce_scatter(dense, voxels, lambda: col.norm_send(squares(voxels, 256), 0))
        fresh = col.norm_wait(0)
        beta = jnp.where(k > 0, fresh / gamma[...], jnp.zeros_like(fresh))
        gamma[...] = fresh
        image[...] = forth + beta * image[...]
        likely = jnp.where(k > 0, guess[...], guess[...] / fresh)

        def start(step):
            if step == 0:
                world.send(squares(image, image.shape[0]))
                direction[...] = search[...] + beta * direction[...]
            if step == col.n_out - 1:
                alpha = fresh / world.wait()
                guess[...] = 1.25 * alpha
                ratio[...] = alpha / likely
                residual_ref[...] -= alpha * image[...]
                volume_ref[...] += alpha * direction[...]

        @pl.when(k + 1 < ITERS)
        def _():
            col.all_gather(residual_ref[...] - likely * image[...], images, start)
            held[...] += ratio[...] * (images[...].astype(F32) - held[...])
            rays[...] = held[...].astype(BF16)

        @pl.when(k + 1 == ITERS)
        def _():
            for step in range(col.n_out):
                start(step)

        return carry

    lax.fori_loop(0, ITERS, iteration, 0)


def axis_scratch(n, n_in, chunk, frames):
    n_out = n // n_in
    dma = pltpu.SemaphoreType.DMA
    near, far = (max(n_in - 1, 1), n_out), (max(n_out - 1, 1),)
    return [
        pltpu.VMEM(near + (chunk, frames), BF16),
        pltpu.VMEM(near + (chunk, frames), BF16),
        pltpu.VMEM(far + (chunk, frames), BF16),
        pltpu.VMEM(far + (chunk, frames), BF16),
        pltpu.VMEM((2, n, 1, frames), F32),
        dma(near), dma(near), dma(far), dma(far), dma(far), dma(far), dma(near), dma(near),
        dma((2, n - 1)), dma((2, n - 1)),
    ]


def line_scratch(n, n_in, chunk, frames):
    dma = pltpu.SemaphoreType.DMA
    near = (max(n_in - 1, 1), 4)
    return [
        pltpu.VMEM(near + (chunk, frames), BF16),
        pltpu.VMEM(near + (chunk, frames), BF16),
        pltpu.VMEM((3, chunk, frames), BF16),
        pltpu.VMEM((4, chunk, frames), BF16),
        pltpu.VMEM((2, n, 1, frames), F32),
        pltpu.VMEM((chunk, frames), F32),
        pltpu.VMEM((chunk, frames), F32),
        dma(near + (PARTS,)), dma(near + (PARTS,)), dma((3, PARTS)), dma((4, PARTS)),
        dma((3, PARTS)), dma((3, PARTS)), dma(near + (PARTS,)), dma(near + (PARTS,)),
        dma((2, n - 1)), dma((2, n - 1)),
    ]


def exchange_scratch(count, rows, frames):
    buffer = pltpu.VMEM((rows, frames), BF16)
    return [buffer] * 4 + [pltpu.SemaphoreType.DMA((count,))] * 6


def finish(volume_ref, residual_ref, volume_out, residual_out, sems):
    copies = [pltpu.make_async_copy(volume_ref, volume_out, sems.at[0]),
              pltpu.make_async_copy(residual_ref, residual_out, sems.at[1])]
    for copy in copies:
        copy.start()
    for copy in copies:
        copy.wait()


def local(n_row, n_col, tiles, tile_row, tile_col, tile_count, sinogram):
    tile, frames = tiles.shape[3], sinogram.shape[2]
    n_rays, n_vox = RT * tile, VT * tile
    vmem = pl.BlockSpec(memory_space=pltpu.VMEM)
    smem = pl.BlockSpec(memory_space=pltpu.SMEM)
    slots = tiles.shape[2]
    col_in = inner_size(n_col)
    vox_piece, ray_piece = n_vox // n_row, n_rays // n_col
    pieces = []
    if n_row == 2 * CORES:
        step = min(PIECE, vox_piece)
        pieces = [(at, step) for at in range(0, 2 * vox_piece, step)]
    hbm = pl.BlockSpec(memory_space=pl.ANY)
    volume, residual = pl.pallas_call(
        functools.partial(cgls_kernel, (n_row, n_col, col_in, pieces)),
        out_shape=(
            jax.ShapeDtypeStruct((vox_piece, frames), F32),
            jax.ShapeDtypeStruct((ray_piece, frames), F32),
        ),
        in_specs=[vmem, vmem, vmem, hbm, vmem],
        out_specs=(vmem, vmem),
        scratch_shapes=[
            pltpu.VMEM((slots + 1, tile, tile), BF16),
            pltpu.VMEM((n_rays, n_vox), BF16),
            pltpu.VMEM((n_vox, n_rays), BF16),
            pltpu.VMEM((n_rays, frames), BF16),
            pltpu.VMEM((n_vox, frames), BF16),
            pltpu.VMEM((n_rays, frames), BF16),
            pltpu.VMEM((n_rays, frames), F32),
            pltpu.VMEM((vox_piece, frames), F32),
            pltpu.VMEM((vox_piece, frames), F32),
            pltpu.VMEM((ray_piece, frames), F32),
            pltpu.VMEM((1, frames), F32),
            pltpu.VMEM((1, frames), F32),
            pltpu.VMEM((1, frames), F32),
            pltpu.SemaphoreType.DMA,
            pltpu.VMEM((RT * VT // slots, 1, slots), jnp.int32),
            pltpu.SMEM((RT * VT // slots, 1, slots), jnp.int32),
            pltpu.SemaphoreType.DMA,
        ]
        + axis_scratch(n_row, CORES, vox_piece, frames)
        + (line_scratch if n_col == 4 * col_in else axis_scratch)(n_col, col_in, ray_piece, frames)
        + [pltpu.VMEM((n_row * n_col, 1, frames), F32)] + [pltpu.SemaphoreType.DMA((n_row * n_col - 1,))] * 2
        + (exchange_scratch(len(pieces), 2 * vox_piece, frames) if pieces else []),
        compiler_params=pltpu.CompilerParams(
            collective_id=0, has_side_effects=True, vmem_limit_bytes=62 * 1024 * 1024
        ),
        name="cgls",
    )(tile_count, tile_row[0], tile_col[0], tiles[0, 0], sinogram[0])
    volume, residual = pl.pallas_call(
        finish,
        out_shape=(
            jax.ShapeDtypeStruct((vox_piece, frames), F32),
            jax.ShapeDtypeStruct((ray_piece, frames), F32),
        ),
        in_specs=[vmem, vmem],
        out_specs=(hbm, hbm),
        scratch_shapes=[pltpu.SemaphoreType.DMA((2,))],
        name="finish",
    )(volume, residual)
    return volume[None], residual[None]


def solution(mesh):
    return jax.shard_map(
        functools.partial(local, mesh.shape["row"], mesh.shape["col"]),
        mesh=mesh,
        in_specs=(
            P("row", "col", None, None, None),
            P("row", "col", None),
            P("row", "col", None),
            P("row", "col"),
            P("row", "col", None),
        ),
        out_specs=(P("col", "row", None), P("row", "col", None)),
        check_vma=False,
    )
```

```python
import functools

import jax
import jax.numpy as jnp
from jax import lax
from jax.experimental import pallas as pl
from jax.experimental.pallas import tpu as pltpu
from jax.sharding import PartitionSpec as P

RT = 16
VT = 16
ITERS = 4
CORES = 2
PIECE = 256
PARTS = 4
AXIS_REFS = 15
LINE_REFS = 17
MESH = pl.DeviceIdType.MESH
F32 = jnp.float32
BF16 = jnp.bfloat16


def inner_size(n):
    size = 1
    while size * 2 * size * 2 <= n and n % (size * 2) == 0:
        size *= 2
    return size


def build(slot_ref, tiles, dense, flipped, start, stop):
    tile = tiles.shape[1]
    group = 4

    def place(step, carry):
        for j in range(group):
            at = step * group + j
            r = pl.multiple_of(at // VT * tile, tile)
            c = pl.multiple_of(lax.rem(at, VT) * tile, tile)
            block = tiles[slot_ref[at // slot_ref.shape[2], 0, lax.rem(at, slot_ref.shape[2])]]
            dense[pl.ds(r, tile), pl.ds(c, tile)] = block
            flipped[pl.ds(c, tile), pl.ds(r, tile)] = block.T
        return carry

    lax.fori_loop(start // group, stop // group, place, 0)


class Axis:
    def __init__(self, name, n, n_in, chunk, refs):
        self.name, self.n, self.n_in, self.n_out, self.chunk = name, n, n_in, n // n_in, chunk
        self.near_out, self.near_in, self.far_out, self.far_in, self.norm_in = refs[:5]
        (self.near_ss, self.near_rs, self.far_ss, self.far_rs, self.out_ss, self.out_rs,
         self.in_ss, self.in_rs, self.norm_ss, self.norm_rs) = refs[5:]
        self.me = lax.axis_index(name)
        self.o, self.i = self.me // n_in, lax.rem(self.me, n_in)

    def index(self, e, d):
        return lax.rem(self.o + e + self.n_out, self.n_out) * self.n_in + lax.rem(self.i + d + self.n_in, self.n_in)

    def rows(self, index):
        return pl.ds(pl.multiple_of(index * self.chunk, self.chunk), self.chunk)

    def send(self, src, dst, ss, rs, index):
        copy = pltpu.make_async_remote_copy(
            src_ref=src, dst_ref=dst, send_sem=ss, recv_sem=rs,
            device_id={self.name: index}, device_id_type=MESH,
        )
        copy.start()
        return copy

    def outer_order(self):
        return sorted(range(1, self.n_out), key=lambda e: -min(e, self.n_out - e)) + [0]

    def reduce_scatter(self, matrix, full, queued=lambda: None):
        def piece(index):
            return jnp.dot(matrix[self.rows(index), :], full[...], preferred_element_type=F32)

        copies = []
        near = {}
        for e in self.outer_order():
            for d in range(1, self.n_in):
                self.near_out[d - 1, e] = piece(self.index(e, d)).astype(BF16)
                near[e, d] = self.send(
                    self.near_out.at[d - 1, e], self.near_in.at[d - 1, e],
                    self.near_ss.at[d - 1, e], self.near_rs.at[d - 1, e], self.index(0, d))
        queued()
        far = {}
        total = None
        for e in self.outer_order():
            total = piece(self.index(e, 0))
            for d in range(1, self.n_in):
                near[e, d].wait_recv()
                total += self.near_in[d - 1, e].astype(F32)
            if e:
                self.far_out[e - 1] = total.astype(BF16)
                far[e] = self.send(
                    self.far_out.at[e - 1], self.far_in.at[e - 1],
                    self.far_ss.at[e - 1], self.far_rs.at[e - 1], self.index(e, 0))
        for e in far:
            far[e].wait_recv()
            total += self.far_in[e - 1].astype(F32)
        for copy in list(near.values()) + list(far.values()):
            copy.wait_send()
        return total

    def all_gather(self, value, full, between=lambda step: None, use=lambda rows: None):
        full[self.rows(self.me), :] = value.astype(BF16)
        mine = full.at[self.rows(self.me), :]
        far, near = {}, {}
        for e in reversed(self.outer_order()[:-1]):
            far[e] = self.send(mine, mine, self.out_ss.at[e - 1], self.out_rs.at[e - 1], self.index(e, 0))
        for d in range(1, self.n_in):
            near[0, d] = self.send(mine, mine, self.in_ss.at[d - 1, 0], self.in_rs.at[d - 1, 0], self.index(0, d))
        between(0)
        for step, e in enumerate(reversed(self.outer_order()[:-1])):
            far[e].wait_recv()
            theirs = full.at[self.rows(self.index(-e, 0)), :]
            for d in range(1, self.n_in):
                near[e, d] = self.send(
                    theirs, theirs, self.in_ss.at[d - 1, e], self.in_rs.at[d - 1, e], self.index(0, d))
            between(step + 1)
        for copy in near.values():
            copy.wait_recv()
        for index in range(self.n):
            use(self.rows(index))
        for copy in list(near.values()) + list(far.values()):
            copy.wait_send()

    def peer(self, d):
        return lax.rem(self.me + d, self.n)

    def norm_send(self, value, which):
        self.norm_in[which, 0] = value
        return [
            self.send(self.norm_in.at[which, 0], self.norm_in.at[which, d],
                      self.norm_ss.at[which, d - 1], self.norm_rs.at[which, d - 1], self.peer(d))
            for d in range(1, self.n)
        ]

    def norm_wait(self, which):
        for d in range(1, self.n):
            pltpu.make_async_remote_copy(
                src_ref=self.norm_in.at[which, 0], dst_ref=self.norm_in.at[which, d],
                send_sem=self.norm_ss.at[which, d - 1], recv_sem=self.norm_rs.at[which, d - 1],
                device_id={self.name: self.peer(d)}, device_id_type=MESH,
            ).wait()
        total = self.norm_in[which, 0]
        for d in range(1, self.n):
            total += self.norm_in[which, d]
        return total


class Line(Axis):
    def __init__(self, name, n, n_in, chunk, refs):
        self.near_out, self.near_in, self.far_out, self.far_in, self.norm_in, self.hold, self.total = refs[:7]
        (self.near_ss, self.near_rs, self.far_ss, self.far_rs, self.out_ss, self.out_rs,
         self.in_ss, self.in_rs, self.norm_ss, self.norm_rs) = refs[7:]
        self.name, self.n, self.n_in, self.n_out, self.chunk = name, n, n_in, n // n_in, chunk
        self.me = lax.axis_index(name)
        self.o, self.i = self.me // n_in, lax.rem(self.me, n_in)
        low = self.o < 2
        self.edge = (self.o == 0) | (self.o == 3)
        self.inner = jnp.logical_not(self.edge)
        self.outer = [self.o, jnp.where(low, 1 - self.o, 5 - self.o), jnp.where(low, 2, 1), jnp.where(low, 3, 0)]
        self.part = chunk // PARTS

    def at(self, place, d=0):
        return self.outer[place] * self.n_in + lax.rem(self.i + d, self.n_in)

    def span(self, h):
        return pl.ds(h * self.part, self.part)

    def block(self, full, place, h):
        start = pl.multiple_of(self.at(place) * self.chunk + h * self.part, self.part)
        return full.at[pl.ds(start, self.part), :]

    def link(self, src, dst, ss, rs, index):
        return pltpu.make_async_remote_copy(
            src_ref=src, dst_ref=dst, send_sem=ss, recv_sem=rs,
            device_id={self.name: index}, device_id_type=MESH,
        )

    def reduce_scatter(self, matrix, full, queued=lambda: None):
        def piece(index):
            return jnp.dot(matrix[self.rows(index), :], full[...], preferred_element_type=F32)

        parts, others = range(PARTS), range(1, self.n_in)
        sent = []
        for place in (3, 2, 1, 0):
            for d in others:
                self.near_out[d - 1, place] = piece(self.at(place, d)).astype(BF16)
                for h in parts:
                    copy = self.link(self.near_out.at[d - 1, place, self.span(h)],
                                     self.near_in.at[d - 1, place, self.span(h)],
                                     self.near_ss.at[d - 1, place, h], self.near_rs.at[d - 1, place, h],
                                     self.at(0, d))
                    copy.start()
                    sent.append(copy)
        queued()

        def gathered(place, h):
            part = self.hold[self.span(h)]
            for d in others:
                self.link(self.near_out.at[d - 1, place, self.span(h)], self.near_in.at[d - 1, place, self.span(h)],
                          self.near_ss.at[d - 1, place, h], self.near_rs.at[d - 1, place, h],
                          self.at(0, d)).wait_recv()
                part += self.near_in[d - 1, place, self.span(h)].astype(F32)
            return part

        def far(which, slot, h, place):
            return self.link(self.far_out.at[which, self.span(h)], self.far_in.at[slot, self.span(h)],
                             self.far_ss.at[which, h], self.far_rs.at[slot, h], self.at(place))

        self.hold[...] = piece(self.at(3))
        for h in parts:
            self.hold[self.span(h)] = gathered(3, h)

            @pl.when(self.edge)
            def _():
                self.far_out[2, self.span(h)] = self.hold[self.span(h)].astype(BF16)
                far(2, 3, h, 1).start()

        self.total[...] = self.hold[...]
        self.hold[...] = piece(self.at(2))
        for h in parts:
            self.far_out[1, self.span(h)] = gathered(2, h).astype(BF16)
            far(1, jnp.where(self.edge, 2, 1), h, 2).start()
        self.hold[...] = piece(self.at(1))

        @pl.when(self.inner)
        def _():
            for h in parts:
                far(2, 3, h, 1).wait_recv()
                value = self.total[self.span(h)] + self.far_in[3, self.span(h)].astype(F32)
                self.far_out[2, self.span(h)] = value.astype(BF16)
                far(2, 1, h, 3).start()

        for h in parts:
            self.far_out[0, self.span(h)] = gathered(1, h).astype(BF16)
            far(0, 0, h, 1).start()
        self.hold[...] = piece(self.at(0))
        for h in parts:
            self.hold[self.span(h)] = gathered(0, h)
        for h in parts:
            far(0, 0, h, 1).wait_recv()
            self.hold[self.span(h)] += self.far_in[0, self.span(h)].astype(F32)

        @pl.when(self.inner)
        def _():
            for h in parts:
                far(1, 2, h, 2).wait_recv()
                self.hold[self.span(h)] += self.far_in[2, self.span(h)].astype(F32)

        for h in parts:
            far(1, 1, h, 2).wait_recv()
            self.hold[self.span(h)] += self.far_in[1, self.span(h)].astype(F32)
        for copy in sent:
            copy.wait_send()
        for which in range(3):
            for h in parts:
                far(which, 0, h, 1).wait_send()
        return self.hold[...]

    def all_gather(self, value, full, between=lambda step: None, use=lambda rows: None):
        parts, others = range(PARTS), range(1, self.n_in)
        full[self.rows(self.me), :] = value.astype(BF16)

        def pass_on(place, slot, to, sem, h):
            block = self.block(full, place, h)
            return self.link(block, block, self.out_ss.at[sem, h], self.out_rs.at[slot - 1, h], self.at(to))

        def arrived(place, h):
            block = self.block(full, place, h)
            self.link(block, block, self.out_ss.at[0, h], self.out_rs.at[place - 1, h], self.at(1)).wait_recv()

        def share(place, h):
            block = self.block(full, place, h)
            return [self.link(block, block, self.in_ss.at[d - 1, place, h], self.in_rs.at[d - 1, place, h],
                              self.at(0, d)) for d in others]

        def spread(place, h):
            for copy in share(place, h):
                copy.start()

        @pl.when(self.edge)
        def _():
            for h in parts:
                pass_on(0, 3, 3, 0, h).start()
            for h in parts:
                pass_on(0, 1, 1, 2, h).start()
                pass_on(0, 3, 2, 1, h).start()

        @pl.when(self.inner)
        def _():
            for h in parts:
                pass_on(0, 2, 2, 0, h).start()
                pass_on(0, 1, 1, 1, h).start()

        for h in parts:
            spread(0, h)
        between(0)

        @pl.when(self.inner)
        def _():
            for h in parts:
                arrived(2, h)
                pass_on(2, 2, 1, 2, h).start()
                spread(2, h)

        for h in parts:
            arrived(1, h)
            spread(1, h)
        between(1)
        for h in parts:
            arrived(3, h)
            spread(3, h)
        between(2)

        @pl.when(self.edge)
        def _():
            for h in parts:
                arrived(2, h)
                spread(2, h)

        between(3)
        for place in range(4):
            use(self.rows(self.at(place)))
        for place in (0, 1, 3, 2):
            for h in parts:
                for copy in share(place, h):
                    copy.wait()
            for d in others:
                use(self.rows(self.at(place, d)))
        for sem in range(3):
            for h in parts:
                pass_on(0, 1, 1, sem, h).wait_send()


class World:
    def __init__(self, row, col, refs):
        self.row, self.col = row, col
        self.got, self.ss, self.rs = refs

    def peers(self):
        for at in range(1, self.row.n * self.col.n):
            a, b = at // self.col.n, at % self.col.n
            yield at, {self.row.name: self.row.peer(a), self.col.name: self.col.peer(b)}

    def copy(self, at, device):
        return pltpu.make_async_remote_copy(
            src_ref=self.got.at[0], dst_ref=self.got.at[at], send_sem=self.ss.at[at - 1],
            recv_sem=self.rs.at[at - 1], device_id=device, device_id_type=MESH)

    def send(self, value):
        self.got[0] = value
        for at, device in self.peers():
            self.copy(at, device).start()

    def wait(self):
        for at, device in self.peers():
            self.copy(at, device).wait()
        return jnp.sum(self.got[...], axis=0)


class Exchange:
    def __init__(self, axis, pieces, refs):
        self.axis, self.pieces = axis, pieces
        self.near_out, self.near_in, self.far_out, self.far_in = refs[:4]
        self.near_ss, self.near_rs, self.far_ss, self.far_rs, self.back_ss, self.back_rs = refs[4:]

    def rows(self, core, at, size):
        chunk = self.axis.chunk
        start = (at // chunk * self.axis.n_in + core) * chunk + at % chunk
        return pl.ds(pl.multiple_of(start, size), size)

    def run(self, matrix, full, total, own):
        axis = self.axis
        mine, other = axis.i, 1 - axis.i
        near_peer, far_peer = axis.index(0, 1), axis.index(1, 0)

        def piece(core, at, size):
            return jnp.dot(matrix[self.rows(core, at, size), :], full[...], preferred_element_type=F32)

        def give(p):
            at, size = self.pieces[p]
            self.near_out[pl.ds(at, size)] = piece(other, at, size).astype(BF16)
            return axis.send(self.near_out.at[pl.ds(at, size)], self.near_in.at[pl.ds(at, size)],
                             self.near_ss.at[p], self.near_rs.at[p], near_peer)

        count = len(self.pieces)
        near, far, back = [give(0)], [], []
        for p, (at, size) in enumerate(self.pieces):
            if p + 1 < count:
                near.append(give(p + 1))
            part = piece(mine, at, size)
            near[p].wait_recv()
            here = pl.ds(at, size)
            self.far_out[here] = (part + self.near_in[here].astype(F32)).astype(BF16)
            far.append(axis.send(self.far_out.at[here], self.far_in.at[here],
                                 self.far_ss.at[p], self.far_rs.at[p], far_peer))
        for p, (at, size) in enumerate(self.pieces):
            far[p].wait_recv()
            here = pl.ds(at, size)
            rows = self.rows(mine, at, size)
            value = self.far_out[here].astype(F32) + self.far_in[here].astype(F32)
            total[rows] = value.astype(BF16)
            back.append(axis.send(total.at[rows], total.at[rows], self.back_ss.at[p], self.back_rs.at[p], near_peer))
        start = pl.multiple_of(axis.o * axis.chunk, axis.chunk)
        here = pl.ds(start, axis.chunk)
        own[...] = self.far_out[here].astype(F32) + self.far_in[here].astype(F32)
        for copy in back:
            copy.wait_recv()

        def settle():
            for copy in near + far + back:
                copy.wait_send()

        return settle


def squares(ref, step):
    total = None
    for at in range(0, ref.shape[0], step):
        part = ref[at:at + step, :].astype(F32)
        part = jnp.sum(part * part, axis=0, keepdims=True)
        total = part if total is None else total + part
    return total


def cgls_kernel(sizes, count_hbm, row_hbm, col_hbm, tiles_hbm, sino_hbm, volume_ref, residual_ref, tiles, dense, flipped, rays, voxels,
                images, held, search, direction, image, gamma, guess, ratio, load_sem, table, slot_ref, table_sem,
                count_ref, row_ref, col_ref, sino_ref, bring_sems, *refs):
    n_row, n_col, col_in, pieces = sizes
    row = Axis("row", n_row, CORES, search.shape[0], refs[:AXIS_REFS])
    kind, count = (Line, LINE_REFS) if n_col == 4 * col_in else (Axis, AXIS_REFS)
    col = kind("col", n_col, col_in, image.shape[0], refs[AXIS_REFS:AXIS_REFS + count])
    refs = refs[AXIS_REFS + count:]
    world = World(row, col, refs[:3])
    exchange = Exchange(row, pieces, refs[3:]) if pieces else None

    barrier = pltpu.get_barrier_semaphore()
    for axis in (row, col):
        for d in range(1, axis.n):
            pl.semaphore_signal(barrier, inc=1, device_id={axis.name: axis.peer(d)}, device_id_type=MESH)
    bring = [pltpu.make_async_copy(src, dst, bring_sems.at[at]) for at, (src, dst) in enumerate(
        ((row_hbm, row_ref), (col_hbm, col_ref), (count_hbm, count_ref), (sino_hbm, sino_ref)))]
    for copy in bring:
        copy.start()
    slots = tiles_hbm.shape[0]
    load = pltpu.make_async_copy(tiles_hbm, tiles.at[pl.ds(0, slots)], load_sem)
    load.start()
    for copy in bring:
        copy.wait()
    tiles[slots] = jnp.zeros(tiles.shape[1:], tiles.dtype)

    place = (row_ref[...] * VT + col_ref[...]).astype(F32)
    place = jnp.broadcast_to(place, (slots, slots)).T
    slot = lax.broadcasted_iota(jnp.int32, (slots, slots), 0)
    lane = lax.broadcasted_iota(jnp.int32, (slots, slots), 1).astype(F32)
    for at in range(0, RT * VT, slots):
        live = (place == lane + at) & (slot < count_ref[...])
        table[at // slots] = jnp.min(jnp.where(live, slot, slots), axis=0, keepdims=True)
    fill = pltpu.make_async_copy(table, slot_ref, table_sem)
    fill.start()

    pl.semaphore_wait(barrier, n_row + n_col - 2)

    share = RT * VT // col.n_out

    def build_share(step):
        if step == 0:
            load.wait()
            fill.wait()
        build(slot_ref, tiles, dense, flipped, step * share, (step + 1) * share)

    def widen(rows):
        held[rows, :] = rays[rows, :].astype(F32)

    col.all_gather(sino_ref[...], rays, build_share, widen)
    residual_ref[...] = sino_ref[...]
    volume_ref[...] = jnp.zeros_like(volume_ref)
    direction[...] = jnp.zeros_like(direction)
    image[...] = jnp.zeros_like(image)
    gamma[...] = jnp.ones_like(gamma)
    row.norm_send(squares(rays, 256), 1)

    def iteration(k, carry):
        if exchange:
            settle = exchange.run(flipped, rays, voxels, search)
        else:
            search[...] = row.reduce_scatter(flipped, rays)
            row.all_gather(search[...], voxels)
            settle = lambda: None

        def queued():
            col.norm_send(squares(voxels, 256), 0)
            settle()

        @pl.when(k == 0)
        def _():
            guess[...] = row.norm_wait(1)

        forth = col.reduce_scatter(dense, voxels, queued)
        fresh = col.norm_wait(0)
        beta = jnp.where(k > 0, fresh / gamma[...], jnp.zeros_like(fresh))
        gamma[...] = fresh
        image[...] = forth + beta * image[...]
        likely = jnp.where(k > 0, guess[...], guess[...] / fresh)

        def start(step):
            if step == 0:
                world.send(squares(image, image.shape[0]))
                direction[...] = search[...] + beta * direction[...]
            if step == col.n_out - 1:
                alpha = fresh / world.wait()
                guess[...] = 1.25 * alpha
                ratio[...] = alpha / likely
                residual_ref[...] -= alpha * image[...]
                volume_ref[...] += alpha * direction[...]

        @pl.when(k + 1 < ITERS)
        def _():
            def use(rows):
                value = held[rows, :]
                value += ratio[...] * (images[rows, :].astype(F32) - value)
                held[rows, :] = value
                rays[rows, :] = value.astype(BF16)

            col.all_gather(residual_ref[...] - likely * image[...], images, start, use)

        @pl.when(k + 1 == ITERS)
        def _():
            for step in range(col.n_out):
                start(step)

        return carry

    lax.fori_loop(0, ITERS, iteration, 0)


def axis_scratch(n, n_in, chunk, frames):
    n_out = n // n_in
    dma = pltpu.SemaphoreType.DMA
    near, far = (max(n_in - 1, 1), n_out), (max(n_out - 1, 1),)
    return [
        pltpu.VMEM(near + (chunk, frames), BF16),
        pltpu.VMEM(near + (chunk, frames), BF16),
        pltpu.VMEM(far + (chunk, frames), BF16),
        pltpu.VMEM(far + (chunk, frames), BF16),
        pltpu.VMEM((2, n, 1, frames), F32),
        dma(near), dma(near), dma(far), dma(far), dma(far), dma(far), dma(near), dma(near),
        dma((2, n - 1)), dma((2, n - 1)),
    ]


def line_scratch(n, n_in, chunk, frames):
    dma = pltpu.SemaphoreType.DMA
    near = (max(n_in - 1, 1), 4)
    return [
        pltpu.VMEM(near + (chunk, frames), BF16),
        pltpu.VMEM(near + (chunk, frames), BF16),
        pltpu.VMEM((3, chunk, frames), BF16),
        pltpu.VMEM((4, chunk, frames), BF16),
        pltpu.VMEM((2, n, 1, frames), F32),
        pltpu.VMEM((chunk, frames), F32),
        pltpu.VMEM((chunk, frames), F32),
        dma(near + (PARTS,)), dma(near + (PARTS,)), dma((3, PARTS)), dma((4, PARTS)),
        dma((3, PARTS)), dma((3, PARTS)), dma(near + (PARTS,)), dma(near + (PARTS,)),
        dma((2, n - 1)), dma((2, n - 1)),
    ]


def exchange_scratch(count, rows, frames):
    buffer = pltpu.VMEM((rows, frames), BF16)
    return [buffer] * 4 + [pltpu.SemaphoreType.DMA((count,))] * 6


def local(n_row, n_col, tiles, tile_row, tile_col, tile_count, sinogram):
    tile, frames = tiles.shape[3], sinogram.shape[2]
    n_rays, n_vox = RT * tile, VT * tile
    vmem = pl.BlockSpec(memory_space=pltpu.VMEM)
    smem = pl.BlockSpec(memory_space=pltpu.SMEM)
    slots = tiles.shape[2]
    col_in = inner_size(n_col)
    vox_piece, ray_piece = n_vox // n_row, n_rays // n_col
    pieces = []
    if n_row == 2 * CORES:
        step = min(PIECE, vox_piece)
        pieces = [(at, step) for at in range(0, 2 * vox_piece, step)]
    hbm = pl.BlockSpec(memory_space=pltpu.HBM)
    volume, residual = pl.pallas_call(
        functools.partial(cgls_kernel, (n_row, n_col, col_in, pieces)),
        out_shape=(pltpu.VMEM((vox_piece, frames), F32), pltpu.VMEM((ray_piece, frames), F32)),
        in_specs=[hbm] * 5,
        out_specs=(vmem, vmem),
        scratch_shapes=[
            pltpu.VMEM((slots + 1, tile, tile), BF16),
            pltpu.VMEM((n_rays, n_vox), BF16),
            pltpu.VMEM((n_vox, n_rays), BF16),
            pltpu.VMEM((n_rays, frames), BF16),
            pltpu.VMEM((n_vox, frames), BF16),
            pltpu.VMEM((n_rays, frames), BF16),
            pltpu.VMEM((n_rays, frames), F32),
            pltpu.VMEM((vox_piece, frames), F32),
            pltpu.VMEM((vox_piece, frames), F32),
            pltpu.VMEM((ray_piece, frames), F32),
            pltpu.VMEM((1, frames), F32),
            pltpu.VMEM((1, frames), F32),
            pltpu.VMEM((1, frames), F32),
            pltpu.SemaphoreType.DMA,
            pltpu.VMEM((RT * VT // slots, 1, slots), jnp.int32),
            pltpu.SMEM((RT * VT // slots, 1, slots), jnp.int32),
            pltpu.SemaphoreType.DMA,
            pltpu.VMEM((1, 1), jnp.int32),
            pltpu.VMEM((1, slots), jnp.int32),
            pltpu.VMEM((1, slots), jnp.int32),
            pltpu.VMEM((ray_piece, frames), F32),
            pltpu.SemaphoreType.DMA((4,)),
        ]
        + axis_scratch(n_row, CORES, vox_piece, frames)
        + (line_scratch if n_col == 4 * col_in else axis_scratch)(n_col, col_in, ray_piece, frames)
        + [pltpu.VMEM((n_row * n_col, 1, frames), F32)] + [pltpu.SemaphoreType.DMA((n_row * n_col - 1,))] * 2
        + (exchange_scratch(len(pieces), 2 * vox_piece, frames) if pieces else []),
        compiler_params=pltpu.CompilerParams(
            collective_id=0, has_side_effects=True, vmem_limit_bytes=62 * 1024 * 1024
        ),
        name="cgls",
    )(tile_count, tile_row[0], tile_col[0], tiles[0, 0], sinogram[0])
    return volume[None], residual[None]


def solution(mesh):
    return jax.shard_map(
        functools.partial(local, mesh.shape["row"], mesh.shape["col"]),
        mesh=mesh,
        in_specs=(
            P("row", "col", None, None, None),
            P("row", "col", None),
            P("row", "col", None),
            P("row", "col"),
            P("row", "col", None),
        ),
        out_specs=(P("col", "row", None), P("row", "col", None)),
        check_vma=False,
    )
```

```python
import functools

import jax
import jax.numpy as jnp
from jax import lax
from jax.experimental import pallas as pl
from jax.experimental.pallas import tpu as pltpu
from jax.sharding import PartitionSpec as P

RT = 16
VT = 16
ITERS = 4
CORES = 2
PIECE = 256
PARTS = 4
AXIS_REFS = 15
LINE_REFS = 17
MESH = pl.DeviceIdType.MESH
F32 = jnp.float32
BF16 = jnp.bfloat16


def inner_size(n):
    size = 1
    while size * 2 * size * 2 <= n and n % (size * 2) == 0:
        size *= 2
    return size


def build(slot_ref, tiles, dense, flipped, start, stop):
    tile = tiles.shape[1]
    group = 4

    def place(step, carry):
        for j in range(group):
            at = step * group + j
            r = pl.multiple_of(at // VT * tile, tile)
            c = pl.multiple_of(lax.rem(at, VT) * tile, tile)
            block = tiles[slot_ref[at // slot_ref.shape[2], 0, lax.rem(at, slot_ref.shape[2])]]
            dense[pl.ds(r, tile), pl.ds(c, tile)] = block
            flipped[pl.ds(c, tile), pl.ds(r, tile)] = block.T
        return carry

    lax.fori_loop(start // group, stop // group, place, 0)


class Axis:
    def __init__(self, name, n, n_in, chunk, refs):
        self.name, self.n, self.n_in, self.n_out, self.chunk = name, n, n_in, n // n_in, chunk
        self.near_out, self.near_in, self.far_out, self.far_in, self.norm_in = refs[:5]
        (self.near_ss, self.near_rs, self.far_ss, self.far_rs, self.out_ss, self.out_rs,
         self.in_ss, self.in_rs, self.norm_ss, self.norm_rs) = refs[5:]
        self.me = lax.axis_index(name)
        self.o, self.i = self.me // n_in, lax.rem(self.me, n_in)

    def index(self, e, d):
        return lax.rem(self.o + e + self.n_out, self.n_out) * self.n_in + lax.rem(self.i + d + self.n_in, self.n_in)

    def rows(self, index):
        return pl.ds(pl.multiple_of(index * self.chunk, self.chunk), self.chunk)

    def send(self, src, dst, ss, rs, index):
        copy = pltpu.make_async_remote_copy(
            src_ref=src, dst_ref=dst, send_sem=ss, recv_sem=rs,
            device_id={self.name: index}, device_id_type=MESH,
        )
        copy.start()
        return copy

    def outer_order(self):
        return sorted(range(1, self.n_out), key=lambda e: -min(e, self.n_out - e)) + [0]

    def reduce_scatter(self, matrix, full, queued=lambda: None):
        def piece(index):
            return jnp.dot(matrix[self.rows(index), :], full[...], preferred_element_type=F32)

        copies = []
        near = {}
        for e in self.outer_order():
            for d in range(1, self.n_in):
                self.near_out[d - 1, e] = piece(self.index(e, d)).astype(BF16)
                near[e, d] = self.send(
                    self.near_out.at[d - 1, e], self.near_in.at[d - 1, e],
                    self.near_ss.at[d - 1, e], self.near_rs.at[d - 1, e], self.index(0, d))
        queued()
        far = {}
        total = None
        for e in self.outer_order():
            total = piece(self.index(e, 0))
            for d in range(1, self.n_in):
                near[e, d].wait_recv()
                total += self.near_in[d - 1, e].astype(F32)
            if e:
                self.far_out[e - 1] = total.astype(BF16)
                far[e] = self.send(
                    self.far_out.at[e - 1], self.far_in.at[e - 1],
                    self.far_ss.at[e - 1], self.far_rs.at[e - 1], self.index(e, 0))
        for e in far:
            far[e].wait_recv()
            total += self.far_in[e - 1].astype(F32)
        for copy in list(near.values()) + list(far.values()):
            copy.wait_send()
        return total

    def all_gather(self, value, full, between=lambda step: None, use=lambda rows: None):
        full[self.rows(self.me), :] = value.astype(BF16)
        mine = full.at[self.rows(self.me), :]
        far, near = {}, {}
        for e in reversed(self.outer_order()[:-1]):
            far[e] = self.send(mine, mine, self.out_ss.at[e - 1], self.out_rs.at[e - 1], self.index(e, 0))
        for d in range(1, self.n_in):
            near[0, d] = self.send(mine, mine, self.in_ss.at[d - 1, 0], self.in_rs.at[d - 1, 0], self.index(0, d))
        between(0)
        for step, e in enumerate(reversed(self.outer_order()[:-1])):
            far[e].wait_recv()
            theirs = full.at[self.rows(self.index(-e, 0)), :]
            for d in range(1, self.n_in):
                near[e, d] = self.send(
                    theirs, theirs, self.in_ss.at[d - 1, e], self.in_rs.at[d - 1, e], self.index(0, d))
            between(step + 1)
        for copy in near.values():
            copy.wait_recv()
        for index in range(self.n):
            use(self.rows(index))
        for copy in list(near.values()) + list(far.values()):
            copy.wait_send()

    def peer(self, d):
        return lax.rem(self.me + d, self.n)

    def norm_send(self, value, which):
        self.norm_in[which, 0] = value
        return [
            self.send(self.norm_in.at[which, 0], self.norm_in.at[which, d],
                      self.norm_ss.at[which, d - 1], self.norm_rs.at[which, d - 1], self.peer(d))
            for d in range(1, self.n)
        ]

    def norm_wait(self, which):
        for d in range(1, self.n):
            pltpu.make_async_remote_copy(
                src_ref=self.norm_in.at[which, 0], dst_ref=self.norm_in.at[which, d],
                send_sem=self.norm_ss.at[which, d - 1], recv_sem=self.norm_rs.at[which, d - 1],
                device_id={self.name: self.peer(d)}, device_id_type=MESH,
            ).wait()
        total = self.norm_in[which, 0]
        for d in range(1, self.n):
            total += self.norm_in[which, d]
        return total


class Line(Axis):
    def __init__(self, name, n, n_in, chunk, refs):
        self.near_out, self.near_in, self.far_out, self.far_in, self.norm_in, self.hold, self.kept = refs[:7]
        (self.near_ss, self.near_rs, self.far_ss, self.far_rs, self.out_ss, self.out_rs,
         self.in_ss, self.in_rs, self.norm_ss, self.norm_rs) = refs[7:]
        self.name, self.n, self.n_in, self.n_out, self.chunk = name, n, n_in, n // n_in, chunk
        self.me = lax.axis_index(name)
        self.o, self.i = self.me // n_in, lax.rem(self.me, n_in)
        low = self.o < 2
        self.edge = (self.o == 0) | (self.o == 3)
        self.inner = jnp.logical_not(self.edge)
        self.outer = [self.o, jnp.where(low, 1 - self.o, 5 - self.o), jnp.where(low, 2, 1), jnp.where(low, 3, 0)]
        self.part = chunk // PARTS

    def at(self, place, d=0):
        return self.outer[place] * self.n_in + lax.rem(self.i + d, self.n_in)

    def span(self, h):
        return pl.ds(h * self.part, self.part)

    def block(self, full, place, h):
        start = pl.multiple_of(self.at(place) * self.chunk + h * self.part, self.part)
        return full.at[pl.ds(start, self.part), :]

    def link(self, src, dst, ss, rs, index):
        return pltpu.make_async_remote_copy(
            src_ref=src, dst_ref=dst, send_sem=ss, recv_sem=rs,
            device_id={self.name: index}, device_id_type=MESH,
        )

    def reduce_scatter(self, matrix, full, queued=lambda: None):
        def piece(index):
            return jnp.dot(matrix[self.rows(index), :], full[...], preferred_element_type=F32)

        parts, others = range(PARTS), range(1, self.n_in)
        sent = []
        for place in (3, 2, 1, 0):
            for d in others:
                self.near_out[d - 1, place] = piece(self.at(place, d)).astype(BF16)
                for h in parts:
                    copy = self.link(self.near_out.at[d - 1, place, self.span(h)],
                                     self.near_in.at[d - 1, place, self.span(h)],
                                     self.near_ss.at[d - 1, place, h], self.near_rs.at[d - 1, place, h],
                                     self.at(0, d))
                    copy.start()
                    sent.append(copy)
        queued()

        def gathered(place, h):
            part = self.kept[place, self.span(h)]
            for d in others:
                self.link(self.near_out.at[d - 1, place, self.span(h)], self.near_in.at[d - 1, place, self.span(h)],
                          self.near_ss.at[d - 1, place, h], self.near_rs.at[d - 1, place, h],
                          self.at(0, d)).wait_recv()
                part += self.near_in[d - 1, place, self.span(h)].astype(F32)
            return part

        def far(which, slot, h, place):
            return self.link(self.far_out.at[which, self.span(h)], self.far_in.at[slot, self.span(h)],
                             self.far_ss.at[which, h], self.far_rs.at[slot, h], self.at(place))

        for place in (3, 2, 1, 0):
            self.kept[place] = piece(self.at(place))
        for h in parts:
            self.kept[3, self.span(h)] = gathered(3, h)

            @pl.when(self.edge)
            def _():
                self.far_out[2, self.span(h)] = self.kept[3, self.span(h)].astype(BF16)
                far(2, 3, h, 1).start()

        for h in parts:
            self.far_out[1, self.span(h)] = gathered(2, h).astype(BF16)
            far(1, jnp.where(self.edge, 2, 1), h, 2).start()

        for h in parts:
            self.far_out[0, self.span(h)] = gathered(1, h).astype(BF16)
            far(0, 0, h, 1).start()

        @pl.when(self.inner)
        def _():
            for h in parts:
                far(2, 3, h, 1).wait_recv()
                value = self.kept[3, self.span(h)] + self.far_in[3, self.span(h)].astype(F32)
                self.far_out[2, self.span(h)] = value.astype(BF16)
                far(2, 1, h, 3).start()

        for h in parts:
            self.hold[self.span(h)] = gathered(0, h)
        for h in parts:
            far(0, 0, h, 1).wait_recv()
            self.hold[self.span(h)] += self.far_in[0, self.span(h)].astype(F32)

        @pl.when(self.inner)
        def _():
            for h in parts:
                far(1, 2, h, 2).wait_recv()
                self.hold[self.span(h)] += self.far_in[2, self.span(h)].astype(F32)

        for h in parts:
            far(1, 1, h, 2).wait_recv()
            self.hold[self.span(h)] += self.far_in[1, self.span(h)].astype(F32)
        for copy in sent:
            copy.wait_send()
        for which in range(3):
            for h in parts:
                far(which, 0, h, 1).wait_send()
        return self.hold[...]

    def all_gather(self, value, full, between=lambda step: None, use=lambda rows: None):
        parts, others = range(PARTS), range(1, self.n_in)
        full[self.rows(self.me), :] = value.astype(BF16)

        def pass_on(place, slot, to, sem, h):
            block = self.block(full, place, h)
            return self.link(block, block, self.out_ss.at[sem, h], self.out_rs.at[slot - 1, h], self.at(to))

        def arrived(place, h):
            block = self.block(full, place, h)
            self.link(block, block, self.out_ss.at[0, h], self.out_rs.at[place - 1, h], self.at(1)).wait_recv()

        def share(place, h):
            block = self.block(full, place, h)
            return [self.link(block, block, self.in_ss.at[d - 1, place, h], self.in_rs.at[d - 1, place, h],
                              self.at(0, d)) for d in others]

        def spread(place, h):
            for copy in share(place, h):
                copy.start()

        @pl.when(self.edge)
        def _():
            for h in parts:
                pass_on(0, 3, 3, 0, h).start()
            for h in parts:
                pass_on(0, 1, 1, 2, h).start()
                pass_on(0, 3, 2, 1, h).start()

        @pl.when(self.inner)
        def _():
            for h in parts:
                pass_on(0, 2, 2, 0, h).start()
                pass_on(0, 1, 1, 1, h).start()

        for h in parts:
            spread(0, h)
        between(0)

        @pl.when(self.inner)
        def _():
            for h in parts:
                arrived(2, h)
                pass_on(2, 2, 1, 2, h).start()
                spread(2, h)

        for h in parts:
            arrived(1, h)
            spread(1, h)
        between(1)
        for h in parts:
            arrived(3, h)
            spread(3, h)
        between(2)

        @pl.when(self.edge)
        def _():
            for h in parts:
                arrived(2, h)
                spread(2, h)

        between(3)
        for place in range(4):
            use(self.rows(self.at(place)))
        for place in (0, 1, 3, 2):
            for h in parts:
                for copy in share(place, h):
                    copy.wait()
            for d in others:
                use(self.rows(self.at(place, d)))
        for sem in range(3):
            for h in parts:
                pass_on(0, 1, 1, sem, h).wait_send()


class World:
    def __init__(self, row, col, refs):
        self.row, self.col = row, col
        self.got, self.ss, self.rs = refs

    def peers(self):
        for at in range(1, self.row.n * self.col.n):
            a, b = at // self.col.n, at % self.col.n
            yield at, {self.row.name: self.row.peer(a), self.col.name: self.col.peer(b)}

    def copy(self, at, device):
        return pltpu.make_async_remote_copy(
            src_ref=self.got.at[0], dst_ref=self.got.at[at], send_sem=self.ss.at[at - 1],
            recv_sem=self.rs.at[at - 1], device_id=device, device_id_type=MESH)

    def send(self, value):
        self.got[0] = value
        for at, device in self.peers():
            self.copy(at, device).start()

    def wait(self):
        for at, device in self.peers():
            self.copy(at, device).wait()
        return jnp.sum(self.got[...], axis=0)


class Exchange:
    def __init__(self, axis, pieces, refs):
        self.axis, self.pieces = axis, pieces
        self.near_out, self.near_in, self.far_out, self.far_in = refs[:4]
        self.near_ss, self.near_rs, self.far_ss, self.far_rs, self.back_ss, self.back_rs = refs[4:]

    def rows(self, core, at, size):
        chunk = self.axis.chunk
        start = (at // chunk * self.axis.n_in + core) * chunk + at % chunk
        return pl.ds(pl.multiple_of(start, size), size)

    def run(self, matrix, full, total, own):
        axis = self.axis
        mine, other = axis.i, 1 - axis.i
        near_peer, far_peer = axis.index(0, 1), axis.index(1, 0)

        def piece(core, at, size):
            return jnp.dot(matrix[self.rows(core, at, size), :], full[...], preferred_element_type=F32)

        def give(p):
            at, size = self.pieces[p]
            self.near_out[pl.ds(at, size)] = piece(other, at, size).astype(BF16)
            return axis.send(self.near_out.at[pl.ds(at, size)], self.near_in.at[pl.ds(at, size)],
                             self.near_ss.at[p], self.near_rs.at[p], near_peer)

        count = len(self.pieces)
        near, far, back = [give(0)], [], []
        for p, (at, size) in enumerate(self.pieces):
            if p + 1 < count:
                near.append(give(p + 1))
            part = piece(mine, at, size)
            near[p].wait_recv()
            here = pl.ds(at, size)
            self.far_out[here] = (part + self.near_in[here].astype(F32)).astype(BF16)
            far.append(axis.send(self.far_out.at[here], self.far_in.at[here],
                                 self.far_ss.at[p], self.far_rs.at[p], far_peer))
        for p, (at, size) in enumerate(self.pieces):
            far[p].wait_recv()
            here = pl.ds(at, size)
            rows = self.rows(mine, at, size)
            value = self.far_out[here].astype(F32) + self.far_in[here].astype(F32)
            total[rows] = value.astype(BF16)
            back.append(axis.send(total.at[rows], total.at[rows], self.back_ss.at[p], self.back_rs.at[p], near_peer))
        start = pl.multiple_of(axis.o * axis.chunk, axis.chunk)
        here = pl.ds(start, axis.chunk)
        own[...] = self.far_out[here].astype(F32) + self.far_in[here].astype(F32)
        for copy in back:
            copy.wait_recv()

        def settle():
            for copy in near + far + back:
                copy.wait_send()

        return settle


def squares(ref, step):
    total = None
    for at in range(0, ref.shape[0], step):
        part = ref[at:at + step, :].astype(F32)
        part = jnp.sum(part * part, axis=0, keepdims=True)
        total = part if total is None else total + part
    return total


def cgls_kernel(sizes, count_hbm, row_hbm, col_hbm, tiles_hbm, sino_hbm, volume_ref, residual_ref, tiles, dense, flipped, rays, voxels,
                images, held, search, direction, image, gamma, guess, ratio, load_sem, table, slot_ref, table_sem,
                count_ref, row_ref, col_ref, sino_ref, bring_sems, *refs):
    n_row, n_col, col_in, pieces = sizes
    row = Axis("row", n_row, CORES, search.shape[0], refs[:AXIS_REFS])
    kind, count = (Line, LINE_REFS) if n_col == 4 * col_in else (Axis, AXIS_REFS)
    col = kind("col", n_col, col_in, image.shape[0], refs[AXIS_REFS:AXIS_REFS + count])
    refs = refs[AXIS_REFS + count:]
    world = World(row, col, refs[:3])
    exchange = Exchange(row, pieces, refs[3:]) if pieces else None

    barrier = pltpu.get_barrier_semaphore()
    for axis in (row, col):
        for d in range(1, axis.n):
            pl.semaphore_signal(barrier, inc=1, device_id={axis.name: axis.peer(d)}, device_id_type=MESH)
    bring = [pltpu.make_async_copy(src, dst, bring_sems.at[at]) for at, (src, dst) in enumerate(
        ((row_hbm, row_ref), (col_hbm, col_ref), (count_hbm, count_ref), (sino_hbm, sino_ref)))]
    for copy in bring:
        copy.start()
    slots = tiles_hbm.shape[0]
    load = pltpu.make_async_copy(tiles_hbm, tiles.at[pl.ds(0, slots)], load_sem)
    load.start()
    for copy in bring:
        copy.wait()
    tiles[slots] = jnp.zeros(tiles.shape[1:], tiles.dtype)

    place = (row_ref[...] * VT + col_ref[...]).astype(F32)
    place = jnp.broadcast_to(place, (slots, slots)).T
    slot = lax.broadcasted_iota(jnp.int32, (slots, slots), 0)
    lane = lax.broadcasted_iota(jnp.int32, (slots, slots), 1).astype(F32)
    for at in range(0, RT * VT, slots):
        live = (place == lane + at) & (slot < count_ref[...])
        table[at // slots] = jnp.min(jnp.where(live, slot, slots), axis=0, keepdims=True)
    fill = pltpu.make_async_copy(table, slot_ref, table_sem)
    fill.start()

    pl.semaphore_wait(barrier, n_row + n_col - 2)

    share = RT * VT // col.n_out

    def build_share(step):
        if step == 0:
            load.wait()
            fill.wait()
        build(slot_ref, tiles, dense, flipped, step * share, (step + 1) * share)

    def widen(rows):
        held[rows, :] = rays[rows, :].astype(F32)

    col.all_gather(sino_ref[...], rays, build_share, widen)
    residual_ref[...] = sino_ref[...]
    volume_ref[...] = jnp.zeros_like(volume_ref)
    direction[...] = jnp.zeros_like(direction)
    image[...] = jnp.zeros_like(image)
    gamma[...] = jnp.ones_like(gamma)
    row.norm_send(squares(rays, 256), 1)

    def iteration(k, carry):
        if exchange:
            settle = exchange.run(flipped, rays, voxels, search)
        else:
            search[...] = row.reduce_scatter(flipped, rays)
            row.all_gather(search[...], voxels)
            settle = lambda: None

        def queued():
            col.norm_send(squares(voxels, 256), 0)
            settle()

        @pl.when(k == 0)
        def _():
            guess[...] = row.norm_wait(1)

        forth = col.reduce_scatter(dense, voxels, queued)
        fresh = col.norm_wait(0)
        beta = jnp.where(k > 0, fresh / gamma[...], jnp.zeros_like(fresh))
        gamma[...] = fresh
        image[...] = forth + beta * image[...]
        likely = jnp.where(k > 0, guess[...], guess[...] / fresh)

        def start(step):
            if step == 0:
                world.send(squares(image, image.shape[0]))
                direction[...] = search[...] + beta * direction[...]
            if step == col.n_out - 1:
                alpha = fresh / world.wait()
                guess[...] = 1.25 * alpha
                ratio[...] = alpha / likely
                residual_ref[...] -= alpha * image[...]
                volume_ref[...] += alpha * direction[...]

        @pl.when(k + 1 < ITERS)
        def _():
            def use(rows):
                value = held[rows, :]
                value += ratio[...] * (images[rows, :].astype(F32) - value)
                held[rows, :] = value
                rays[rows, :] = value.astype(BF16)

            col.all_gather(residual_ref[...] - likely * image[...], images, start, use)

        @pl.when(k + 1 == ITERS)
        def _():
            for step in range(col.n_out):
                start(step)

        return carry

    lax.fori_loop(0, ITERS, iteration, 0)


def axis_scratch(n, n_in, chunk, frames):
    n_out = n // n_in
    dma = pltpu.SemaphoreType.DMA
    near, far = (max(n_in - 1, 1), n_out), (max(n_out - 1, 1),)
    return [
        pltpu.VMEM(near + (chunk, frames), BF16),
        pltpu.VMEM(near + (chunk, frames), BF16),
        pltpu.VMEM(far + (chunk, frames), BF16),
        pltpu.VMEM(far + (chunk, frames), BF16),
        pltpu.VMEM((2, n, 1, frames), F32),
        dma(near), dma(near), dma(far), dma(far), dma(far), dma(far), dma(near), dma(near),
        dma((2, n - 1)), dma((2, n - 1)),
    ]


def line_scratch(n, n_in, chunk, frames):
    dma = pltpu.SemaphoreType.DMA
    near = (max(n_in - 1, 1), 4)
    return [
        pltpu.VMEM(near + (chunk, frames), BF16),
        pltpu.VMEM(near + (chunk, frames), BF16),
        pltpu.VMEM((3, chunk, frames), BF16),
        pltpu.VMEM((4, chunk, frames), BF16),
        pltpu.VMEM((2, n, 1, frames), F32),
        pltpu.VMEM((chunk, frames), F32),
        pltpu.VMEM((4, chunk, frames), F32),
        dma(near + (PARTS,)), dma(near + (PARTS,)), dma((3, PARTS)), dma((4, PARTS)),
        dma((3, PARTS)), dma((3, PARTS)), dma(near + (PARTS,)), dma(near + (PARTS,)),
        dma((2, n - 1)), dma((2, n - 1)),
    ]


def exchange_scratch(count, rows, frames):
    buffer = pltpu.VMEM((rows, frames), BF16)
    return [buffer] * 4 + [pltpu.SemaphoreType.DMA((count,))] * 6


def local(n_row, n_col, tiles, tile_row, tile_col, tile_count, sinogram):
    tile, frames = tiles.shape[3], sinogram.shape[2]
    n_rays, n_vox = RT * tile, VT * tile
    vmem = pl.BlockSpec(memory_space=pltpu.VMEM)
    smem = pl.BlockSpec(memory_space=pltpu.SMEM)
    slots = tiles.shape[2]
    col_in = inner_size(n_col)
    vox_piece, ray_piece = n_vox // n_row, n_rays // n_col
    pieces = []
    if n_row == 2 * CORES:
        step = min(PIECE, vox_piece)
        pieces = [(at, step) for at in range(0, 2 * vox_piece - step, step)]
        pieces += [(2 * vox_piece - at, step // 2) for at in (step, step // 2)]
    hbm = pl.BlockSpec(memory_space=pltpu.HBM)
    volume, residual = pl.pallas_call(
        functools.partial(cgls_kernel, (n_row, n_col, col_in, pieces)),
        out_shape=(pltpu.VMEM((vox_piece, frames), F32), pltpu.VMEM((ray_piece, frames), F32)),
        in_specs=[hbm] * 5,
        out_specs=(vmem, vmem),
        scratch_shapes=[
            pltpu.VMEM((slots + 1, tile, tile), BF16),
            pltpu.VMEM((n_rays, n_vox), BF16),
            pltpu.VMEM((n_vox, n_rays), BF16),
            pltpu.VMEM((n_rays, frames), BF16),
            pltpu.VMEM((n_vox, frames), BF16),
            pltpu.VMEM((n_rays, frames), BF16),
            pltpu.VMEM((n_rays, frames), F32),
            pltpu.VMEM((vox_piece, frames), F32),
            pltpu.VMEM((vox_piece, frames), F32),
            pltpu.VMEM((ray_piece, frames), F32),
            pltpu.VMEM((1, frames), F32),
            pltpu.VMEM((1, frames), F32),
            pltpu.VMEM((1, frames), F32),
            pltpu.SemaphoreType.DMA,
            pltpu.VMEM((RT * VT // slots, 1, slots), jnp.int32),
            pltpu.SMEM((RT * VT // slots, 1, slots), jnp.int32),
            pltpu.SemaphoreType.DMA,
            pltpu.VMEM((1, 1), jnp.int32),
            pltpu.VMEM((1, slots), jnp.int32),
            pltpu.VMEM((1, slots), jnp.int32),
            pltpu.VMEM((ray_piece, frames), F32),
            pltpu.SemaphoreType.DMA((4,)),
        ]
        + axis_scratch(n_row, CORES, vox_piece, frames)
        + (line_scratch if n_col == 4 * col_in else axis_scratch)(n_col, col_in, ray_piece, frames)
        + [pltpu.VMEM((n_row * n_col, 1, frames), F32)] + [pltpu.SemaphoreType.DMA((n_row * n_col - 1,))] * 2
        + (exchange_scratch(len(pieces), 2 * vox_piece, frames) if pieces else []),
        compiler_params=pltpu.CompilerParams(
            collective_id=0, has_side_effects=True, vmem_limit_bytes=62 * 1024 * 1024
        ),
        name="cgls",
    )(tile_count, tile_row[0], tile_col[0], tiles[0, 0], sinogram[0])
    return volume[None], residual[None]


def solution(mesh):
    return jax.shard_map(
        functools.partial(local, mesh.shape["row"], mesh.shape["col"]),
        mesh=mesh,
        in_specs=(
            P("row", "col", None, None, None),
            P("row", "col", None),
            P("row", "col", None),
            P("row", "col"),
            P("row", "col", None),
        ),
        out_specs=(P("col", "row", None), P("row", "col", None)),
        check_vma=False,
    )
```
